32 devices in a mesh: seq: 4 (over y, x), batch: 8 (over z, core).
Axes of the slice: x: 2, y: 2, z: 4, core: 2. Of those that a mesh axis runs over, the one named last changes fastest.
Arguments:
- activations: bfloat16 [8, 3072, 4096], P('batch', 'seq'), may hold values from -18 to 18
- out_grads: bfloat16 [8, 3072, 4096], P('batch', 'seq'), may hold values from -0.29882812 to 0.29882812
- lengths: int32 [8, 3], P('batch'), may hold values from 1 to 1536, 3072 in all within a row
Outputs:
- act_factor: float32 [4096, 4096], P(('seq', 'batch'))
- grad_factor: float32 [4096, 4096], P(('seq', 'batch'))
The draws below stay inside these ranges and needn't reach their ends.
Inputs may be any that keep to these rules, and one draw needn't show every extreme that they name: `lengths`: each row sums to 3072 and its largest entry is exactly 1536.
All inputs are finite; a program needn't handle non-finite values.
Results may differ from the reference program's by a relative error of at most 0.004.
Values may be sent and summed in bfloat16 or wider, within the bound.
No kernel may reach another device: no remote copies, remote signals or barrier semaphores. Data moves between devices by JAX's collectives and lax.ppermute only.
A program may use at most 64 MiB of HBM per device.

```python
import math
import jax
import jax.numpy as jnp
import numpy as np
from jax import lax

D = 4096
SEQS = 3
GROUP_TOK = 3072
MOST = 1536
GROUPS = 8
TOTAL_SEQS = 24


def with_spikes(values, stream_key, source, target, shards_of, factor):
    def block_of(dim):
        return (jnp.arange(values.shape[dim]) // (values.shape[dim] // shards_of)).reshape((-1,) + (1,) * (values.ndim - 1 - dim))

    one_side = jax.random.permutation(stream_key, shards_of)[block_of(target)]
    far = (block_of(target) + shards_of // 2) % shards_of
    return jnp.where((block_of(source) == one_side) | (block_of(source) == far), factor * values, values)


def shard_levels(own_key, extent, shards, least, high):
    def one(dim, shards_of):
        heights = jax.random.uniform(jax.random.fold_in(jax.random.fold_in(own_key, 6), dim), (shards_of,), jnp.float32, least / len(shards), high / len(shards))
        return jnp.repeat(jnp.exp(heights), extent[dim] // shards_of).reshape((-1,) + (1,) * (len(extent) - dim - 1))

    gain = one(*shards[0])
    for cut in shards[1:]:
        gain = gain * one(*cut)
    return gain


def split_up(count, total, reach, skew):
    weights = [(1 << 20) // math.isqrt(grade ** skew) + 1 for grade in range(2, count + 1)]
    rest, given = total - reach - (count - 1), [1] * (count - 1)
    while rest > 0:
        free = [i for i in range(count - 1) if given[i] < reach]
        mass, remaining = sum([weights[i] for i in free]), rest
        for i in free:
            more = min(reach - given[i], max(1, remaining * weights[i] // mass), rest)
            given[i] = given[i] + more
            rest = rest - more
    return np.array([reach] + given)


def uneven(key, number_of, total, reach, skew):
    if number_of == 2:
        one = jax.random.randint(key, (), max(1, total - reach), min(reach, total - 1) + 1)
        return jnp.stack([one, total - one])
    sizes = jnp.asarray(split_up(number_of, total, reach, skew), jnp.int32)
    twos = (number_of - 1) // 2
    source_of, taker = sizes[1:1 + 2 * twos:2], sizes[2:2 + 2 * twos:2]
    margin = jnp.minimum(source_of - 1, reach - taker)
    shifted = jax.random.randint(jax.random.fold_in(key, 1), (twos,), 0, 1 << 20) % (margin + 1)
    sizes = sizes.at[1:1 + 2 * twos:2].set(source_of - shifted).at[2:2 + 2 * twos:2].set(taker + shifted)
    return sizes[jax.random.permutation(jax.random.fold_in(key, 2), number_of)]


def bell_draw_with(stream_key, shape, width, most, split, heavy, held_as=jnp.bfloat16):
    array = width * jax.random.normal(stream_key, shape, jnp.float32)
    if split:
        array = array * shard_levels(stream_key, shape, split, -0.22, 0.18)
    return jnp.clip(with_spikes(array, jax.random.fold_in(stream_key, 3), *heavy), -most, most).astype(held_as)


def setup_inputs(seed: int = 0) -> dict:
    seeds = jax.random.split(jax.random.key(seed), 4)
    activations = bell_draw_with(seeds[0], (GROUPS, GROUP_TOK, D), 3.0, 18.0, ((0, 8), (1, 4)), (0, 2, 8, 2.0))
    out_grads = bell_draw_with(seeds[1], (GROUPS, GROUP_TOK, D), 0.05, 0.29882812, ((0, 8), (1, 4)), (0, 2, 8, 2.0))
    lengths = jax.vmap(lambda own: uneven(own, SEQS, GROUP_TOK, MOST, 2))(jax.random.split(seeds[2], GROUPS)).reshape((GROUPS, SEQS)).astype(jnp.int32)
    return dict(activations=activations, out_grads=out_grads, lengths=lengths)


def reference(activations, out_grads, lengths):
    ends = jnp.cumsum(lengths, axis=1).astype(jnp.int32)
    starts = ends - lengths
    position = jnp.arange(GROUP_TOK, dtype=jnp.int32)

    def reduce_group(item):
        act_group, grad_group, first, last = item
        member = (position[None, :] >= first[:, None]) & (position[None, :] < last[:, None])
        member = member.astype(jnp.bfloat16)
        act_sum = jnp.dot(member, act_group, preferred_element_type=jnp.float32)
        grad_sum = jnp.dot(member, grad_group, preferred_element_type=jnp.float32)
        return act_sum, grad_sum

    act_sum, grad_sum = lax.map(reduce_group, (activations, out_grads, starts, ends))
    act_rows = (act_sum / lengths[:, :, None].astype(jnp.float32)).astype(jnp.bfloat16).reshape(TOTAL_SEQS, D)
    grad_rows = grad_sum.astype(jnp.bfloat16).reshape(TOTAL_SEQS, D)
    act_factor = jnp.dot(act_rows.T, act_rows, preferred_element_type=jnp.float32) / TOTAL_SEQS
    grad_factor = jnp.dot(grad_rows.T, grad_rows, preferred_element_type=jnp.float32) / TOTAL_SEQS
    return act_factor, grad_factor
```

```python
import functools

import jax
import jax.numpy as jnp
from jax import lax
from jax.experimental import pallas as pl
from jax.experimental.pallas import tpu as pltpu
from jax.sharding import Mesh
from jax.sharding import PartitionSpec as P

LANES = 128
ROWS = 8


def spare_split(rows, width):
    spare = ROWS - rows
    if spare <= 0 or rows % spare or (width * rows) % (ROWS * LANES):
        return width, 0
    kept = width * rows // ROWS
    tail = width - kept
    if tail % LANES:
        return width, 0
    return kept, tail


def peers(count):
    return list(range(count - 1, -1, -1))


def partner(index, offset, count):
    if count & (count - 1) == 0:
        return index ^ offset
    return (index + offset) % count


def segment_kernel(seq_count, chunk_count, slabs, act, grad, lens, *refs):
    outs = refs[:chunk_count]
    act_buf, grad_buf, len_buf, act_sem, grad_sem, len_sem = refs[chunk_count:]
    tokens = act.shape[1]
    slab = act_buf.shape[2]
    width = outs[0].shape[1]
    me = lax.axis_index("seq")
    len_copy = pltpu.make_async_copy(lens, len_buf, len_sem)
    len_copy.start()
    copies = []
    for slot, offset in enumerate(peers(chunk_count)):
        base = partner(me, offset, chunk_count) * width
        for part in range(slabs):
            at = slot * slabs + part
            cols = pl.ds(pl.multiple_of(base + part * slab, slab), slab)
            pair = (
                pltpu.make_async_copy(act.at[0, :, cols], act_buf.at[at], act_sem.at[at]),
                pltpu.make_async_copy(grad.at[0, :, cols], grad_buf.at[at], grad_sem.at[at]),
            )
            for copy in pair:
                copy.start()
            copies.append(pair)
    len_copy.wait()
    row = lax.broadcasted_iota(jnp.int32, (ROWS, tokens), 0)
    position = lax.broadcasted_iota(jnp.int32, (ROWS, tokens), 1) + me * tokens
    low = jnp.zeros((ROWS, tokens), jnp.int32)
    high = jnp.zeros((ROWS, tokens), jnp.int32)
    start = jnp.int32(0)
    for s in range(seq_count):
        end = start + len_buf[0, s]
        mine = (row == s) | (row == s + seq_count)
        low = jnp.where(mine, start, low)
        high = jnp.where(mine, end, high)
        start = end
    member = (position >= low) & (position < high)
    act_member = jnp.where(member & (row < seq_count), 1.0, 0.0).astype(jnp.bfloat16)
    grad_member = jnp.where(member & (row >= seq_count), 1.0, 0.0).astype(jnp.bfloat16)
    for slot, offset in enumerate(peers(chunk_count)):
        for part in range(slabs):
            at = slot * slabs + part
            for copy in copies[at]:
                copy.wait()
            sums = jnp.dot(act_member, act_buf[at], preferred_element_type=jnp.float32)
            sums += jnp.dot(grad_member, grad_buf[at], preferred_element_type=jnp.float32)
            outs[offset][:, part * slab : (part + 1) * slab] = sums


def rows_kernel(seq_count, kept, tail, lens, *refs):
    parts, out = refs[:-1], refs[-1]
    total = parts[0][...]
    for part in parts[1:]:
        total += part[...]
    rows = 2 * seq_count
    row = lax.broadcasted_iota(jnp.int32, (ROWS, 1), 0)
    count = jnp.ones((ROWS, 1), jnp.float32)
    for s in range(seq_count):
        count = jnp.where(row == s, lens[0, s].astype(jnp.float32), count)
    total = total / count
    if tail:
        spare = ROWS - rows
        per = rows // spare
        body = total[:, :kept]
        pieces = []
        for k in range(per):
            piece = jnp.zeros((ROWS, tail), jnp.float32)
            for j in range(spare):
                source = total[j * per + k : j * per + k + 1, kept:]
                piece = jnp.where(row == rows + j, source, piece)
            pieces.append(piece)
        packed = jnp.where(row >= rows, jnp.concatenate(pieces, axis=1), body)
    else:
        packed = total
    packed = packed.astype(jnp.bfloat16)
    for g in range(out.shape[0]):
        out[g] = packed


def factor_kernel(seq_count, total_seqs, kept, tail, near, far, act_out, grad_out, stack):
    chunks, pairs = near.shape[0], near.shape[1]
    rows = 2 * seq_count
    width = kept + tail
    half = pairs * ROWS
    row = lax.broadcasted_iota(jnp.int32, (1, ROWS, 1), 1)
    for side, ref in enumerate((near, far)):
        for c in range(chunks):
            block = ref[c]
            at = slice(side * half, (side + 1) * half)
            stack[at, c * width : c * width + kept] = block.reshape(half, kept)
            if tail:
                spare = ROWS - rows
                per = rows // spare
                wide = block.astype(jnp.float32)
                rest = jnp.zeros((pairs, ROWS, tail), jnp.float32)
                for j in range(spare):
                    for k in range(per):
                        source = wide[:, rows + j : rows + j + 1, k * tail : (k + 1) * tail]
                        rest = jnp.where(row == j * per + k, source, rest)
                stack[at, c * width + kept : (c + 1) * width] = rest.astype(jnp.bfloat16).reshape(half, tail)
    tile = act_out.shape[0]
    span = max(tile, LANES)
    me = (lax.axis_index("seq") * lax.axis_size("pair") + lax.axis_index("pair")) * lax.axis_size("core") + lax.axis_index("core")
    first = me * tile
    base = pl.multiple_of(first // LANES * LANES, LANES)
    left = stack[:, pl.ds(base, span)].astype(jnp.float32)
    if tile < span:
        left = pltpu.roll(left, span - (first - base), 1)
    kind = lax.rem(lax.broadcasted_iota(jnp.int32, left.shape, 0), ROWS)
    act_left = jnp.where(kind < seq_count, left, 0.0).astype(jnp.bfloat16)
    grad_left = jnp.where((kind >= seq_count) & (kind < rows), left, 0.0).astype(jnp.bfloat16)
    dims = (((0,), (0,)), ((), ()))
    for out, lhs in ((act_out, act_left), (grad_out, grad_left)):
        product = lax.dot_general(lhs[:, :tile], stack[...], dims, preferred_element_type=jnp.float32)
        out[...] = product * (1.0 / total_seqs)


def local(activations, out_grads, lengths):
    chunks = lax.axis_size("seq")
    pairs = lax.axis_size("pair")
    cores = lax.axis_size("core")
    tokens, depth = activations.shape[1], activations.shape[2]
    seq_count = lengths.shape[1]
    width = depth // chunks
    slabs = 2 if width % (2 * LANES) == 0 else 1
    slab = width // slabs
    devices = chunks * pairs * cores
    tile = depth // devices
    kept, tail = spare_split(2 * seq_count, width)
    vmem = pl.BlockSpec(memory_space=pltpu.VMEM)
    anywhere = pl.BlockSpec(memory_space=pl.ANY)

    parts = pl.pallas_call(
        functools.partial(segment_kernel, seq_count, chunks, slabs),
        out_shape=[jax.ShapeDtypeStruct((ROWS, width), jnp.float32)] * chunks,
        in_specs=[anywhere] * 3,
        out_specs=[vmem] * chunks,
        scratch_shapes=[
            pltpu.VMEM((chunks * slabs, tokens, slab), jnp.bfloat16),
            pltpu.VMEM((chunks * slabs, tokens, slab), jnp.bfloat16),
            pltpu.SMEM(lengths.shape, jnp.int32),
            pltpu.SemaphoreType.DMA((chunks * slabs,)),
            pltpu.SemaphoreType.DMA((chunks * slabs,)),
            pltpu.SemaphoreType.DMA,
        ],
        name="segment_sums",
    )(activations, out_grads, lengths)

    arrived = [parts[0]]
    for offset in peers(chunks)[:-1]:
        ring = [(i, partner(i, offset, chunks)) for i in range(chunks)]
        arrived.append(lax.ppermute(parts[offset], "seq", ring))

    spread = pl.pallas_call(
        functools.partial(rows_kernel, seq_count, kept, tail),
        out_shape=jax.ShapeDtypeStruct((chunks * pairs, ROWS, kept), jnp.bfloat16),
        in_specs=[pl.BlockSpec(memory_space=pltpu.SMEM)] + [vmem] * chunks,
        out_specs=vmem,
        name="mean_rows",
    )(lengths, *arrived)

    near = lax.all_to_all(spread, ("seq", "pair"), 0, 0, tiled=True)
    far = lax.ppermute(near, "core", [(i, (i + 1) % cores) for i in range(cores)])
    near, far = (a.reshape(chunks, pairs, ROWS, kept) for a in (near, far))

    return pl.pallas_call(
        functools.partial(factor_kernel, seq_count, seq_count * pairs * cores, kept, tail),
        out_shape=[jax.ShapeDtypeStruct((tile, depth), jnp.float32)] * 2,
        in_specs=[vmem] * 2,
        out_specs=[vmem] * 2,
        scratch_shapes=[pltpu.VMEM((2 * pairs * ROWS, depth), jnp.bfloat16)],
        name="factor_tiles",
    )(near, far)


def solution(mesh):
    batch = mesh.shape["batch"]
    split = Mesh(mesh.devices.reshape(mesh.shape["seq"], batch // 2, 2), ("seq", "pair", "core"))
    groups = ("pair", "core")
    in_specs = (P(groups, "seq", None), P(groups, "seq", None), P(groups, None))
    out_specs = (P(("seq",) + groups, None), P(("seq",) + groups, None))

    def program(activations, out_grads, lengths):
        return tuple(jax.shard_map(local, mesh=split, in_specs=in_specs, out_specs=out_specs, check_vma=False)(activations, out_grads, lengths))

    return program
```

```python
import functools

import jax
import jax.numpy as jnp
from jax import lax
from jax.experimental import pallas as pl
from jax.experimental.pallas import tpu as pltpu
from jax.sharding import Mesh
from jax.sharding import PartitionSpec as P

LANES = 128
ROWS = 8
MIB = 1 << 20


def spare_split(rows, width):
    spare = ROWS - rows
    if spare <= 0 or rows % spare or (width * rows) % (ROWS * LANES):
        return width, 0
    kept = width * rows // ROWS
    tail = width - kept
    if tail % LANES:
        return width, 0
    return kept, tail


def partner(index, offset, count):
    if count & (count - 1) == 0:
        return index ^ offset
    return (index + offset) % count


def fold(values, rows, kept, tail):
    if not tail:
        return values
    row = lax.broadcasted_iota(jnp.int32, (ROWS, 1), 0)
    spare = ROWS - rows
    per = rows // spare
    pieces = []
    for k in range(per):
        piece = values[:, k * tail : (k + 1) * tail]
        for j in range(spare):
            piece = jnp.where(row == rows + j, values[j * per + k : j * per + k + 1, kept:], piece)
        pieces.append(piece)
    return jnp.concatenate(pieces, axis=1)


def unfold(block, rows, kept, tail):
    row = lax.broadcasted_iota(jnp.int32, (1, ROWS, 1), 1)
    spare = ROWS - rows
    per = rows // spare
    wide = block.astype(jnp.float32)
    rest = jnp.zeros((block.shape[0], ROWS, tail), jnp.float32)
    for j in range(spare):
        for k in range(per):
            source = wide[:, rows + j : rows + j + 1, k * tail : (k + 1) * tail]
            rest = jnp.where(row == j * per + k, source, rest)
    return rest.astype(block.dtype)


def segment_kernel(seq_count, chunk_count, offsets, slabs, kept, tail, act, grad, lens, *refs):
    outs = refs[: len(offsets)]
    act_buf, grad_buf, len_buf, act_sem, grad_sem, len_sem = refs[len(offsets) :]
    tokens = act.shape[1]
    slab = act_buf.shape[2]
    width = kept + tail
    rows = 2 * seq_count
    me = lax.axis_index("seq")
    len_copy = pltpu.make_async_copy(lens, len_buf, len_sem)
    len_copy.start()
    copies = []
    for slot, offset in enumerate(offsets):
        base = partner(me, offset, chunk_count) * width
        for part in range(slabs):
            at = slot * slabs + part
            cols = pl.ds(pl.multiple_of(base + part * slab, slab), slab)
            pair = (
                pltpu.make_async_copy(act.at[0, :, cols], act_buf.at[at], act_sem.at[at]),
                pltpu.make_async_copy(grad.at[0, :, cols], grad_buf.at[at], grad_sem.at[at]),
            )
            for copy in pair:
                copy.start()
            copies.append(pair)
    len_copy.wait()
    row = lax.broadcasted_iota(jnp.int32, (ROWS, tokens), 0)
    position = lax.broadcasted_iota(jnp.int32, (ROWS, tokens), 1) + me * tokens
    thin = lax.broadcasted_iota(jnp.int32, (ROWS, 1), 0)
    low = jnp.zeros((ROWS, tokens), jnp.int32)
    high = jnp.zeros((ROWS, tokens), jnp.int32)
    count = jnp.ones((ROWS, 1), jnp.float32)
    start = jnp.int32(0)
    for s in range(seq_count):
        size = len_buf[0, s]
        mine = (row == s) | (row == s + seq_count)
        low = jnp.where(mine, start, low)
        high = jnp.where(mine, start + size, high)
        count = jnp.where(thin == s, size.astype(jnp.float32), count)
        start = start + size
    member = (position >= low) & (position < high)
    act_member = jnp.where(member & (row < seq_count), 1.0, 0.0).astype(jnp.bfloat16)
    grad_member = jnp.where(member & (row >= seq_count), 1.0, 0.0).astype(jnp.bfloat16)
    for slot in range(len(offsets)):
        sums = []
        for part in range(slabs):
            at = slot * slabs + part
            for copy in copies[at]:
                copy.wait()
            both = jnp.dot(act_member, act_buf[at], preferred_element_type=jnp.float32)
            both += jnp.dot(grad_member, grad_buf[at], preferred_element_type=jnp.float32)
            sums.append(both)
        outs[slot][...] = fold(jnp.concatenate(sums, axis=1) / count, rows, kept, tail)


def spread_kernel(*refs):
    parts, out = refs[:-1], refs[-1]
    total = parts[0][...]
    for part in parts[1:]:
        total += part[...]
    total = total.astype(out.dtype)
    for g in range(out.shape[0]):
        out[g] = total


def factor_kernel(seq_count, total_seqs, kept, tail, near, far, act_out, grad_out, own, act_buf, grad_buf, act_sem, grad_sem):
    chunks, pairs = near.shape[0], near.shape[1]
    rows = 2 * seq_count
    width = kept + tail
    half = pairs * ROWS
    tile, piece = act_buf.shape[1:]

    def chunk(c):
        parts = []
        for ref in (near, far):
            block = ref[c]
            flat = block.reshape(half, kept)
            if tail:
                flat = jnp.concatenate([flat, unfold(block, rows, kept, tail).reshape(half, tail)], axis=1)
            parts.append(flat)
        return jnp.concatenate(parts, axis=0)

    seq = lax.axis_index("seq")
    own[...] = chunk(seq).astype(jnp.float32)
    first = (lax.axis_index("pair") * lax.axis_size("core") + lax.axis_index("core")) * tile
    span = max(tile, LANES)
    base = pl.multiple_of(first // LANES * LANES, LANES)
    left = own[:, pl.ds(base, span)]
    if tile < span:
        left = pltpu.roll(left, span - (first - base), 1)
    left = left.T[:tile]
    kind = lax.rem(lax.broadcasted_iota(jnp.int32, left.shape, 1), ROWS)
    act_left = jnp.where(kind < seq_count, left, 0.0)
    grad_left = jnp.where((kind >= seq_count) & (kind < rows), left, 0.0)
    left = jnp.concatenate([act_left, grad_left], axis=0).astype(jnp.bfloat16)
    copies = []
    for c in range(chunks):
        right = chunk(c)
        for part in range(width // piece):
            at = c * (width // piece) + part
            product = jnp.dot(left, right[:, part * piece : (part + 1) * piece], preferred_element_type=jnp.float32)
            product *= 1.0 / total_seqs
            act_buf[at] = product[:tile]
            grad_buf[at] = product[tile:]
            cols = pl.ds(at * piece, piece)
            pair = (
                pltpu.make_async_copy(act_buf.at[at], act_out.at[:, cols], act_sem.at[at]),
                pltpu.make_async_copy(grad_buf.at[at], grad_out.at[:, cols], grad_sem.at[at]),
            )
            for copy in pair:
                copy.start()
            copies.append(pair)
    for pair in copies:
        for copy in pair:
            copy.wait()


def local(activations, out_grads, lengths):
    chunks = lax.axis_size("seq")
    pairs = lax.axis_size("pair")
    cores = lax.axis_size("core")
    tokens, depth = activations.shape[1], activations.shape[2]
    seq_count = lengths.shape[1]
    width = depth // chunks
    slabs = 2 if width % (2 * LANES) == 0 else 1
    slab = width // slabs
    tile = depth // (chunks * pairs * cores)
    kept, tail = spare_split(2 * seq_count, width)
    vmem = pl.BlockSpec(memory_space=pltpu.VMEM)
    anywhere = pl.BlockSpec(memory_space=pl.ANY)
    held = [pltpu.with_memory_space_constraint(a, pltpu.HBM) for a in (activations, out_grads, lengths)]

    def segment_sums(offsets):
        count = len(offsets) * slabs
        return pl.pallas_call(
            functools.partial(segment_kernel, seq_count, chunks, offsets, slabs, kept, tail),
            out_shape=[jax.ShapeDtypeStruct((ROWS, kept), jnp.float32)] * len(offsets),
            in_specs=[anywhere] * 3,
            out_specs=[vmem] * len(offsets),
            scratch_shapes=[
                pltpu.VMEM((count, tokens, slab), jnp.bfloat16),
                pltpu.VMEM((count, tokens, slab), jnp.bfloat16),
                pltpu.SMEM(lengths.shape, jnp.int32),
                pltpu.SemaphoreType.DMA((count,)),
                pltpu.SemaphoreType.DMA((count,)),
                pltpu.SemaphoreType.DMA,
            ],
            compiler_params=pltpu.CompilerParams(vmem_limit_bytes=20 * MIB),
            cost_estimate=pl.CostEstimate(
                flops=4 * ROWS * tokens * width * len(offsets),
                bytes_accessed=4 * tokens * width * len(offsets),
                transcendentals=0,
            ),
            name="segment_sums",
        )(*held)

    offsets = list(range(chunks - 1, 0, -1))
    sent = segment_sums(offsets)
    arrived = []
    for offset, part in zip(offsets, sent):
        ring = [(i, partner(i, offset, chunks)) for i in range(chunks)]
        arrived.append(lax.ppermute(part, "seq", ring))
    arrived += segment_sums([0])

    spread = pl.pallas_call(
        spread_kernel,
        out_shape=jax.ShapeDtypeStruct((chunks * pairs, ROWS, kept), jnp.bfloat16),
        in_specs=[vmem] * chunks,
        out_specs=vmem,
        compiler_params=pltpu.CompilerParams(vmem_limit_bytes=8 * MIB),
        name="mean_rows",
    )(*arrived)

    near = lax.all_to_all(spread, ("seq", "pair"), 0, 0, tiled=True)
    far = lax.ppermute(near, "core", [(i, (i + 1) % cores) for i in range(cores)])
    near, far = (a.reshape(chunks, pairs, ROWS, kept) for a in (near, far))

    piece = slab
    return pl.pallas_call(
        functools.partial(factor_kernel, seq_count, seq_count * pairs * cores, kept, tail),
        out_shape=[jax.ShapeDtypeStruct((tile, depth), jnp.float32)] * 2,
        in_specs=[vmem] * 2,
        out_specs=[anywhere] * 2,
        scratch_shapes=[
            pltpu.VMEM((2 * pairs * ROWS, width), jnp.float32),
            pltpu.VMEM((depth // piece, tile, piece), jnp.float32),
            pltpu.VMEM((depth // piece, tile, piece), jnp.float32),
            pltpu.SemaphoreType.DMA((depth // piece,)),
            pltpu.SemaphoreType.DMA((depth // piece,)),
        ],
        compiler_params=pltpu.CompilerParams(vmem_limit_bytes=20 * MIB),
        name="factor_tiles",
    )(near, far)


def solution(mesh):
    batch = mesh.shape["batch"]
    split = Mesh(mesh.devices.reshape(mesh.shape["seq"], batch // 2, 2), ("seq", "pair", "core"))
    groups = ("pair", "core")
    in_specs = (P(groups, "seq", None), P(groups, "seq", None), P(groups, None))
    out_specs = (P(("seq",) + groups, None), P(("seq",) + groups, None))

    def program(activations, out_grads, lengths):
        return tuple(jax.shard_map(local, mesh=split, in_specs=in_specs, out_specs=out_specs, check_vma=False)(activations, out_grads, lengths))

    return program
```

```python
import functools

import jax
import jax.numpy as jnp
from jax import lax
from jax.experimental import pallas as pl
from jax.experimental.pallas import tpu as pltpu
from jax.sharding import Mesh
from jax.sharding import PartitionSpec as P

LANES = 128
ROWS = 8
MIB = 1 << 20


def spare_split(rows, width):
    spare = ROWS - rows
    if spare <= 0 or rows % spare or (width * rows) % (ROWS * LANES):
        return width, 0
    kept = width * rows // ROWS
    tail = width - kept
    if tail % LANES:
        return width, 0
    return kept, tail


def partner(index, offset, count):
    if count & (count - 1) == 0:
        return index ^ offset
    return (index + offset) % count


def fold(values, rows, kept, tail):
    if not tail:
        return values
    row = lax.broadcasted_iota(jnp.int32, (ROWS, 1), 0)
    spare = ROWS - rows
    per = rows // spare
    pieces = []
    for k in range(per):
        piece = values[:, k * tail : (k + 1) * tail]
        for j in range(spare):
            piece = jnp.where(row == rows + j, values[j * per + k : j * per + k + 1, kept:], piece)
        pieces.append(piece)
    return jnp.concatenate(pieces, axis=1)


def unfold(block, rows, kept, tail):
    row = lax.broadcasted_iota(jnp.int32, (1, ROWS, 1), 1)
    spare = ROWS - rows
    per = rows // spare
    wide = block.astype(jnp.float32)
    rest = jnp.zeros((block.shape[0], ROWS, tail), jnp.float32)
    for j in range(spare):
        for k in range(per):
            source = wide[:, rows + j : rows + j + 1, k * tail : (k + 1) * tail]
            rest = jnp.where(row == j * per + k, source, rest)
    return rest.astype(block.dtype)


def segment_kernel(seq_count, chunk_count, offsets, slabs, kept, tail, act, grad, lens, *refs):
    outs = refs[: len(offsets)]
    act_buf, grad_buf, len_buf, act_sem, grad_sem, len_sem = refs[len(offsets) :]
    tokens = act.shape[1]
    slab = act_buf.shape[1]
    width = kept + tail
    rows = 2 * seq_count
    me = lax.axis_index("seq")
    len_copy = pltpu.make_async_copy(lens, len_buf, len_sem)
    len_copy.start()
    copies = []
    for slot, offset in enumerate(offsets):
        base = partner(me, offset, chunk_count) * width
        cols = pl.ds(pl.multiple_of(base, width), width)
        for part in range(slabs):
            at = slot * slabs + part
            span = pl.ds(part * slab, slab)
            pair = (
                pltpu.make_async_copy(act.at[0, span, cols], act_buf.at[at], act_sem.at[at]),
                pltpu.make_async_copy(grad.at[0, span, cols], grad_buf.at[at], grad_sem.at[at]),
            )
            for copy in pair:
                copy.start()
            copies.append(pair)
    len_copy.wait()
    row = lax.broadcasted_iota(jnp.int32, (ROWS, tokens), 0)
    position = lax.broadcasted_iota(jnp.int32, (ROWS, tokens), 1) + me * tokens
    thin = lax.broadcasted_iota(jnp.int32, (ROWS, 1), 0)
    low = jnp.zeros((ROWS, tokens), jnp.int32)
    high = jnp.zeros((ROWS, tokens), jnp.int32)
    count = jnp.ones((ROWS, 1), jnp.float32)
    start = jnp.int32(0)
    for s in range(seq_count):
        size = len_buf[0, s]
        mine = (row == s) | (row == s + seq_count)
        low = jnp.where(mine, start, low)
        high = jnp.where(mine, start + size, high)
        count = jnp.where(thin == s, size.astype(jnp.float32), count)
        start = start + size
    member = (position >= low) & (position < high)
    act_member = jnp.where(member & (row < seq_count), 1.0, 0.0).astype(jnp.bfloat16)
    grad_member = jnp.where(member & (row >= seq_count), 1.0, 0.0).astype(jnp.bfloat16)
    for slot in range(len(offsets)):
        sums = jnp.zeros((ROWS, width), jnp.float32)
        for part in range(slabs):
            at = slot * slabs + part
            span = slice(part * slab, (part + 1) * slab)
            for member, buf, copy in zip((act_member, grad_member), (act_buf, grad_buf), copies[at]):
                copy.wait()
                sums += jnp.dot(member[:, span], buf[at], preferred_element_type=jnp.float32)
        outs[slot][...] = fold(sums / count, rows, kept, tail)


def spread_kernel(*refs):
    parts, out = refs[:-1], refs[-1]
    total = parts[0][...]
    for part in parts[1:]:
        total += part[...]
    total = total.astype(out.dtype)
    for g in range(out.shape[0]):
        out[g] = total


def factor_kernel(seq_count, total_seqs, kept, tail, near, far, act_out, grad_out, own, act_buf, grad_buf, act_sem, grad_sem):
    chunks, pairs = near.shape[0], near.shape[1]
    rows = 2 * seq_count
    width = kept + tail
    half = pairs * ROWS
    tile, piece = act_buf.shape[1:]

    def chunk(c):
        parts = []
        for ref in (near, far):
            block = ref[chunks - 1 - c]
            flat = block.reshape(half, kept)
            if tail:
                flat = jnp.concatenate([flat, unfold(block, rows, kept, tail).reshape(half, tail)], axis=1)
            parts.append(flat)
        return jnp.concatenate(parts, axis=0)

    seq = lax.axis_index("seq")
    own[...] = chunk(seq).astype(jnp.float32)
    first = (lax.axis_index("pair") * lax.axis_size("core") + lax.axis_index("core")) * tile
    span = max(tile, LANES)
    base = pl.multiple_of(first // LANES * LANES, LANES)
    left = own[:, pl.ds(base, span)]
    if tile < span:
        left = pltpu.roll(left, span - (first - base), 1)
    left = left.T[:tile]
    kind = lax.rem(lax.broadcasted_iota(jnp.int32, left.shape, 1), ROWS)
    act_left = jnp.where(kind < seq_count, left, 0.0)
    grad_left = jnp.where((kind >= seq_count) & (kind < rows), left, 0.0)
    left = jnp.concatenate([act_left, grad_left], axis=0).astype(jnp.bfloat16)
    copies = []
    for c in range(chunks):
        right = chunk(c)
        for part in range(width // piece):
            at = c * (width // piece) + part
            product = jnp.dot(left, right[:, part * piece : (part + 1) * piece], preferred_element_type=jnp.float32)
            product *= 1.0 / total_seqs
            act_buf[at] = product[:tile]
            grad_buf[at] = product[tile:]
            cols = pl.ds(at * piece, piece)
            pair = (
                pltpu.make_async_copy(act_buf.at[at], act_out.at[:, cols], act_sem.at[at]),
                pltpu.make_async_copy(grad_buf.at[at], grad_out.at[:, cols], grad_sem.at[at]),
            )
            for copy in pair:
                copy.start()
            copies.append(pair)
    for pair in copies:
        for copy in pair:
            copy.wait()


def local(activations, out_grads, lengths):
    chunks = lax.axis_size("seq")
    pairs = lax.axis_size("pair")
    cores = lax.axis_size("core")
    tokens, depth = activations.shape[1], activations.shape[2]
    seq_count = lengths.shape[1]
    width = depth // chunks
    slabs = next(n for n in (2, 1) if tokens % (n * LANES) == 0 or n == 1)
    slab = tokens // slabs
    tile = depth // (chunks * pairs * cores)
    kept, tail = spare_split(2 * seq_count, width)
    vmem = pl.BlockSpec(memory_space=pltpu.VMEM)
    anywhere = pl.BlockSpec(memory_space=pl.ANY)
    held = [pltpu.with_memory_space_constraint(a, pltpu.HBM) for a in (activations, out_grads, lengths)]

    def segment_sums(offsets):
        count = len(offsets) * slabs
        return pl.pallas_call(
            functools.partial(segment_kernel, seq_count, chunks, offsets, slabs, kept, tail),
            out_shape=[jax.ShapeDtypeStruct((ROWS, kept), jnp.float32)] * len(offsets),
            in_specs=[anywhere] * 3,
            out_specs=[vmem] * len(offsets),
            scratch_shapes=[
                pltpu.VMEM((count, slab, width), jnp.bfloat16),
                pltpu.VMEM((count, slab, width), jnp.bfloat16),
                pltpu.SMEM(lengths.shape, jnp.int32),
                pltpu.SemaphoreType.DMA((count,)),
                pltpu.SemaphoreType.DMA((count,)),
                pltpu.SemaphoreType.DMA,
            ],
            compiler_params=pltpu.CompilerParams(vmem_limit_bytes=20 * MIB),
            cost_estimate=pl.CostEstimate(
                flops=4 * ROWS * tokens * width * len(offsets),
                bytes_accessed=4 * tokens * width * len(offsets),
                transcendentals=0,
            ),
            name="segment_sums",
        )(*held)

    offsets = list(range(chunks - 1, 0, -1))
    sent = segment_sums(offsets)
    arrived = []
    for offset, part in zip(offsets, sent):
        ring = [(i, partner(i, offset, chunks)) for i in range(chunks)]
        arrived.append(lax.ppermute(part, "seq", ring))
    arrived += segment_sums([0])

    spread = pl.pallas_call(
        spread_kernel,
        out_shape=jax.ShapeDtypeStruct((chunks * pairs, ROWS, kept), jnp.bfloat16),
        in_specs=[vmem] * chunks,
        out_specs=vmem,
        compiler_params=pltpu.CompilerParams(vmem_limit_bytes=8 * MIB),
        name="mean_rows",
    )(*arrived)

    order = list(range(pairs - 1, -1, -2)) + list(range(pairs - 2, -1, -2))
    members = [[(s * pairs + p) * cores + c for s in range(chunks - 1, -1, -1) for p in order] for c in range(cores)]
    near = lax.all_to_all(spread, ("seq", "pair", "core"), 0, 0, axis_index_groups=members, tiled=True)
    far = lax.ppermute(near, "core", [(i, (i + 1) % cores) for i in range(cores)])
    near, far = (a.reshape(chunks, pairs, ROWS, kept) for a in (near, far))

    piece = width // 2 if width % (2 * LANES) == 0 else width
    return pl.pallas_call(
        functools.partial(factor_kernel, seq_count, seq_count * pairs * cores, kept, tail),
        out_shape=[jax.ShapeDtypeStruct((tile, depth), jnp.float32)] * 2,
        in_specs=[vmem] * 2,
        out_specs=[anywhere] * 2,
        scratch_shapes=[
            pltpu.VMEM((2 * pairs * ROWS, width), jnp.float32),
            pltpu.VMEM((depth // piece, tile, piece), jnp.float32),
            pltpu.VMEM((depth // piece, tile, piece), jnp.float32),
            pltpu.SemaphoreType.DMA((depth // piece,)),
            pltpu.SemaphoreType.DMA((depth // piece,)),
        ],
        compiler_params=pltpu.CompilerParams(vmem_limit_bytes=20 * MIB),
        name="factor_tiles",
    )(near, far)


def solution(mesh):
    batch = mesh.shape["batch"]
    split = Mesh(mesh.devices.reshape(mesh.shape["seq"], batch // 2, 2), ("seq", "pair", "core"))
    groups = ("pair", "core")
    in_specs = (P(groups, "seq", None), P(groups, "seq", None), P(groups, None))
    out_specs = (P(("seq",) + groups, None), P(("seq",) + groups, None))

    def program(activations, out_grads, lengths):
        return tuple(jax.shard_map(local, mesh=split, in_specs=in_specs, out_specs=out_specs, check_vma=False)(activations, out_grads, lengths))

    return program
```

```python
import functools

import jax
import jax.numpy as jnp
from jax import lax
from jax.experimental import pallas as pl
from jax.experimental.pallas import tpu as pltpu
from jax.sharding import Mesh
from jax.sharding import PartitionSpec as P

LANES = 128
ROWS = 8
EVEN, TAPER = (1, 1), (3, 2, 1)
MIB = 1 << 20


def spare_split(rows, width):
    spare = ROWS - rows
    if spare <= 0 or rows % spare or (width * rows) % (ROWS * LANES):
        return width, 0
    kept = width * rows // ROWS
    tail = width - kept
    if tail % LANES:
        return width, 0
    return kept, tail


def spans(total, last):
    shares = TAPER if last else EVEN
    edges = [sum(shares[:i]) * total // sum(shares) // LANES * LANES for i in range(len(shares))] + [total]
    return [(a, b) for a, b in zip(edges, edges[1:]) if b > a]


def partner(index, offset, count):
    if count & (count - 1) == 0:
        return index ^ offset
    return (index + offset) % count


def fold(values, rows, kept, tail):
    if not tail:
        return values
    row = lax.broadcasted_iota(jnp.int32, (ROWS, 1), 0)
    spare = ROWS - rows
    per = rows // spare
    pieces = []
    for k in range(per):
        piece = values[:, k * tail : (k + 1) * tail]
        for j in range(spare):
            piece = jnp.where(row == rows + j, values[j * per + k : j * per + k + 1, kept:], piece)
        pieces.append(piece)
    return jnp.concatenate(pieces, axis=1)


def unfold(block, rows, kept, tail):
    row = lax.broadcasted_iota(jnp.int32, (1, ROWS, 1), 1)
    spare = ROWS - rows
    per = rows // spare
    wide = block.astype(jnp.float32)
    rest = jnp.zeros((block.shape[0], ROWS, tail), jnp.float32)
    for j in range(spare):
        for k in range(per):
            source = wide[:, rows + j : rows + j + 1, k * tail : (k + 1) * tail]
            rest = jnp.where(row == j * per + k, source, rest)
    return rest.astype(block.dtype)


def segment_kernel(seq_count, chunk_count, offsets, slabs, kept, tail, act, grad, lens, *refs):
    outs = refs[: len(offsets)]
    act_buf, grad_buf, len_buf, act_sem, grad_sem, len_sem = refs[len(offsets) :]
    tokens = act.shape[1]
    width = kept + tail
    rows = 2 * seq_count
    me = lax.axis_index("seq")
    len_copy = pltpu.make_async_copy(lens, len_buf, len_sem)
    len_copy.start()
    copies = {}
    for slot, offset in enumerate(offsets):
        base = partner(me, offset, chunk_count) * width
        cols = pl.ds(pl.multiple_of(base, width), width)
        for part, (first, last) in enumerate(spans(tokens, slot == len(offsets) - 1)):
            at = slot * slabs + part
            span = pl.ds(first, last - first)
            pair = (
                pltpu.make_async_copy(act.at[0, span, cols], act_buf.at[slot, span], act_sem.at[at]),
                pltpu.make_async_copy(grad.at[0, span, cols], grad_buf.at[slot, span], grad_sem.at[at]),
            )
            for copy in pair:
                copy.start()
            copies[slot, part] = pair
    len_copy.wait()
    row = lax.broadcasted_iota(jnp.int32, (ROWS, tokens), 0)
    position = lax.broadcasted_iota(jnp.int32, (ROWS, tokens), 1) + me * tokens
    thin = lax.broadcasted_iota(jnp.int32, (ROWS, 1), 0)
    low = jnp.zeros((ROWS, tokens), jnp.int32)
    high = jnp.zeros((ROWS, tokens), jnp.int32)
    count = jnp.ones((ROWS, 1), jnp.float32)
    start = jnp.int32(0)
    for s in range(seq_count):
        size = len_buf[0, s]
        mine = (row == s) | (row == s + seq_count)
        low = jnp.where(mine, start, low)
        high = jnp.where(mine, start + size, high)
        count = jnp.where(thin == s, size.astype(jnp.float32), count)
        start = start + size
    member = (position >= low) & (position < high)
    act_member = jnp.where(member & (row < seq_count), 1.0, 0.0).astype(jnp.bfloat16)
    grad_member = jnp.where(member & (row >= seq_count), 1.0, 0.0).astype(jnp.bfloat16)
    for slot in range(len(offsets)):
        sums = jnp.zeros((ROWS, width), jnp.float32)
        for part, (first, last) in enumerate(spans(tokens, slot == len(offsets) - 1)):
            for member, buf, copy in zip((act_member, grad_member), (act_buf, grad_buf), copies[slot, part]):
                copy.wait()
                sums += jnp.dot(member[:, first:last], buf[slot, first:last], preferred_element_type=jnp.float32)
        outs[slot][...] = fold(sums / count, rows, kept, tail)


def spread_kernel(*refs):
    parts, out = refs[:-1], refs[-1]
    total = parts[0][...]
    for part in parts[1:]:
        total += part[...]
    total = total.astype(out.dtype)
    for g in range(out.shape[0]):
        out[g] = total


def tile_products(seq_count, kept, tail, tile, piece, gathered, own, put):
    chunks, pairs = gathered.shape[0], gathered.shape[1]
    rows = 2 * seq_count
    width = kept + tail
    depth = pairs * ROWS

    def chunk(c):
        block = gathered[chunks - 1 - c]
        flat = block.reshape(depth, kept)
        if tail:
            flat = jnp.concatenate([flat, unfold(block, rows, kept, tail).reshape(depth, tail)], axis=1)
        return flat

    own[...] = chunk(lax.axis_index("seq")).astype(jnp.float32)
    first = (lax.axis_index("pair") * lax.axis_size("core") + lax.axis_index("core")) * tile
    span = max(tile, LANES)
    base = pl.multiple_of(first // LANES * LANES, LANES)
    left = own[:, pl.ds(base, span)]
    if tile < span:
        left = pltpu.roll(left, span - (first - base), 1)
    left = left.T[:tile]
    kind = lax.rem(lax.broadcasted_iota(jnp.int32, left.shape, 1), ROWS)
    act_left = jnp.where(kind < seq_count, left, 0.0)
    grad_left = jnp.where((kind >= seq_count) & (kind < rows), left, 0.0)
    left = jnp.concatenate([act_left, grad_left], axis=0).astype(jnp.bfloat16)
    for c in range(chunks):
        right = chunk(c)
        for part in range(width // piece):
            cols = right[:, part * piece : (part + 1) * piece]
            put(c * (width // piece) + part, jnp.dot(left, cols, preferred_element_type=jnp.float32))


def near_kernel(seq_count, kept, tail, tile, near, share, own):
    def put(at, product):
        share[at] = product

    tile_products(seq_count, kept, tail, tile, share.shape[2], near, own, put)


def far_kernel(seq_count, total_seqs, kept, tail, far, share, act_out, grad_out, own, act_buf, grad_buf, act_sem, grad_sem):
    tile, piece = act_buf.shape[1:]
    copies = []

    def put(at, product):
        product = (product + share[at]) * (1.0 / total_seqs)
        act_buf[at] = product[:tile]
        grad_buf[at] = product[tile:]
        cols = pl.ds(at * piece, piece)
        for buf, out, sem in ((act_buf, act_out, act_sem), (grad_buf, grad_out, grad_sem)):
            copy = pltpu.make_async_copy(buf.at[at], out.at[:, cols], sem.at[at])
            copy.start()
            copies.append(copy)

    tile_products(seq_count, kept, tail, tile, piece, far, own, put)
    for copy in copies:
        copy.wait()


def local(activations, out_grads, lengths):
    chunks = lax.axis_size("seq")
    pairs = lax.axis_size("pair")
    cores = lax.axis_size("core")
    tokens, depth = activations.shape[1], activations.shape[2]
    seq_count = lengths.shape[1]
    width = depth // chunks
    slabs = len(TAPER)
    tile = depth // (chunks * pairs * cores)
    kept, tail = spare_split(2 * seq_count, width)
    vmem = pl.BlockSpec(memory_space=pltpu.VMEM)
    anywhere = pl.BlockSpec(memory_space=pl.ANY)
    held = [pltpu.with_memory_space_constraint(a, pltpu.HBM) for a in (activations, out_grads, lengths)]

    def segment_sums(offsets):
        count = len(offsets) * slabs
        return pl.pallas_call(
            functools.partial(segment_kernel, seq_count, chunks, offsets, slabs, kept, tail),
            out_shape=[jax.ShapeDtypeStruct((ROWS, kept), jnp.float32)] * len(offsets),
            in_specs=[anywhere] * 3,
            out_specs=[vmem] * len(offsets),
            scratch_shapes=[
                pltpu.VMEM((len(offsets), tokens, width), jnp.bfloat16),
                pltpu.VMEM((len(offsets), tokens, width), jnp.bfloat16),
                pltpu.SMEM(lengths.shape, jnp.int32),
                pltpu.SemaphoreType.DMA((count,)),
                pltpu.SemaphoreType.DMA((count,)),
                pltpu.SemaphoreType.DMA,
            ],
            compiler_params=pltpu.CompilerParams(vmem_limit_bytes=20 * MIB),
            cost_estimate=pl.CostEstimate(
                flops=4 * ROWS * tokens * width * len(offsets),
                bytes_accessed=4 * tokens * width * len(offsets),
                transcendentals=0,
            ),
            name="segment_sums",
        )(*held)

    offsets = list(range(chunks - 1, 0, -1))
    sent = segment_sums(offsets)
    arrived = []
    for offset, part in zip(offsets, sent):
        ring = [(i, partner(i, offset, chunks)) for i in range(chunks)]
        arrived.append(lax.ppermute(part, "seq", ring))
    arrived += segment_sums([0])

    spread = pl.pallas_call(
        spread_kernel,
        out_shape=jax.ShapeDtypeStruct((chunks * pairs, ROWS, kept), jnp.bfloat16),
        in_specs=[vmem] * chunks,
        out_specs=vmem,
        compiler_params=pltpu.CompilerParams(vmem_limit_bytes=8 * MIB),
        name="mean_rows",
    )(*arrived)

    order = list(range(pairs - 1, -1, -2)) + list(range(pairs - 2, -1, -2))
    members = [[(s * pairs + p) * cores + c for s in range(chunks - 1, -1, -1) for p in order] for c in range(cores)]
    near = lax.all_to_all(spread, ("seq", "pair", "core"), 0, 0, axis_index_groups=members, tiled=True)
    far = lax.ppermute(near, "core", [(i, (i + 1) % cores) for i in range(cores)])
    near, far = (a.reshape(chunks, pairs, ROWS, kept) for a in (near, far))

    piece = width // 2 if width % (2 * LANES) == 0 else width
    pieces = depth // piece
    share = pl.pallas_call(
        functools.partial(near_kernel, seq_count, kept, tail, tile),
        out_shape=jax.ShapeDtypeStruct((pieces, 2 * tile, piece), jnp.float32),
        in_specs=[vmem],
        out_specs=vmem,
        scratch_shapes=[pltpu.VMEM((pairs * ROWS, width), jnp.float32)],
        compiler_params=pltpu.CompilerParams(vmem_limit_bytes=16 * MIB),
        cost_estimate=pl.CostEstimate(
            flops=4 * tile * depth * pairs * ROWS, bytes_accessed=8 * tile * depth, transcendentals=0
        ),
        name="near_share",
    )(near)
    return pl.pallas_call(
        functools.partial(far_kernel, seq_count, seq_count * pairs * cores, kept, tail),
        out_shape=[jax.ShapeDtypeStruct((tile, depth), jnp.float32)] * 2,
        in_specs=[vmem] * 2,
        out_specs=[anywhere] * 2,
        scratch_shapes=[
            pltpu.VMEM((pairs * ROWS, width), jnp.float32),
            pltpu.VMEM((pieces, tile, piece), jnp.float32),
            pltpu.VMEM((pieces, tile, piece), jnp.float32),
            pltpu.SemaphoreType.DMA((pieces,)),
            pltpu.SemaphoreType.DMA((pieces,)),
        ],
        compiler_params=pltpu.CompilerParams(vmem_limit_bytes=20 * MIB),
        name="factor_tiles",
    )(far, share)


def solution(mesh):
    batch = mesh.shape["batch"]
    split = Mesh(mesh.devices.reshape(mesh.shape["seq"], batch // 2, 2), ("seq", "pair", "core"))
    groups = ("pair", "core")
    in_specs = (P(groups, "seq", None), P(groups, "seq", None), P(groups, None))
    out_specs = (P(("seq",) + groups, None), P(("seq",) + groups, None))

    def program(activations, out_grads, lengths):
        return tuple(jax.shard_map(local, mesh=split, in_specs=in_specs, out_specs=out_specs, check_vma=False)(activations, out_grads, lengths))

    return program
```

```python
import functools

import jax
import jax.numpy as jnp
from jax import lax
from jax.experimental import pallas as pl
from jax.experimental.pallas import tpu as pltpu
from jax.sharding import Mesh
from jax.sharding import PartitionSpec as P

LANES = 128
ROWS = 8
EVEN, TAPER = (1, 1), (3, 2, 1)
MIB = 1 << 20


def spare_split(rows, width):
    spare = ROWS - rows
    if spare <= 0 or rows % spare or (width * rows) % (ROWS * LANES):
        return width, 0
    kept = width * rows // ROWS
    tail = width - kept
    if tail % LANES:
        return width, 0
    return kept, tail


def spans(total, last):
    shares = TAPER if last else EVEN
    edges = [sum(shares[:i]) * total // sum(shares) // LANES * LANES for i in range(len(shares))] + [total]
    return [(a, b) for a, b in zip(edges, edges[1:]) if b > a]


def partner(index, offset, count):
    if count & (count - 1) == 0:
        return index ^ offset
    return (index + offset) % count


def fold(values, rows, kept, tail):
    if not tail:
        return values
    row = lax.broadcasted_iota(jnp.int32, (ROWS, 1), 0)
    spare = ROWS - rows
    per = rows // spare
    pieces = []
    for k in range(per):
        piece = values[:, k * tail : (k + 1) * tail]
        for j in range(spare):
            piece = jnp.where(row == rows + j, values[j * per + k : j * per + k + 1, kept:], piece)
        pieces.append(piece)
    return jnp.concatenate(pieces, axis=1)


def unfold(block, rows, kept, tail):
    row = lax.broadcasted_iota(jnp.int32, (1, ROWS, 1), 1)
    spare = ROWS - rows
    per = rows // spare
    wide = block.astype(jnp.float32)
    rest = jnp.zeros((block.shape[0], ROWS, tail), jnp.float32)
    for j in range(spare):
        for k in range(per):
            source = wide[:, rows + j : rows + j + 1, k * tail : (k + 1) * tail]
            rest = jnp.where(row == j * per + k, source, rest)
    return rest.astype(block.dtype)


def segment_kernel(seq_count, chunk_count, offsets, slabs, kept, tail, act, grad, lens, *refs):
    outs = refs[: len(offsets)]
    act_buf, grad_buf, len_buf, act_sem, grad_sem, len_sem = refs[len(offsets) :]
    tokens = act.shape[1]
    width = kept + tail
    rows = 2 * seq_count
    me = lax.axis_index("seq")
    len_copy = pltpu.make_async_copy(lens, len_buf, len_sem)
    len_copy.start()
    copies = {}
    for slot, offset in enumerate(offsets):
        base = partner(me, offset, chunk_count) * width
        cols = pl.ds(pl.multiple_of(base, width), width)
        for part, (first, last) in enumerate(spans(tokens, slot == len(offsets) - 1)):
            at = slot * slabs + part
            span = pl.ds(first, last - first)
            pair = (
                pltpu.make_async_copy(act.at[0, span, cols], act_buf.at[slot, span], act_sem.at[at]),
                pltpu.make_async_copy(grad.at[0, span, cols], grad_buf.at[slot, span], grad_sem.at[at]),
            )
            for copy in pair:
                copy.start()
            copies[slot, part] = pair
    len_copy.wait()
    row = lax.broadcasted_iota(jnp.int32, (ROWS, tokens), 0)
    position = lax.broadcasted_iota(jnp.int32, (ROWS, tokens), 1) + me * tokens
    thin = lax.broadcasted_iota(jnp.int32, (ROWS, 1), 0)
    low = jnp.zeros((ROWS, tokens), jnp.int32)
    high = jnp.zeros((ROWS, tokens), jnp.int32)
    count = jnp.ones((ROWS, 1), jnp.float32)
    start = jnp.int32(0)
    for s in range(seq_count):
        size = len_buf[0, s]
        mine = (row == s) | (row == s + seq_count)
        low = jnp.where(mine, start, low)
        high = jnp.where(mine, start + size, high)
        count = jnp.where(thin == s, size.astype(jnp.float32), count)
        start = start + size
    member = (position >= low) & (position < high)
    act_member = jnp.where(member & (row < seq_count), 1.0, 0.0).astype(jnp.bfloat16)
    grad_member = jnp.where(member & (row >= seq_count), 1.0, 0.0).astype(jnp.bfloat16)
    for slot in range(len(offsets)):
        sums = jnp.zeros((ROWS, width), jnp.float32)
        for part, (first, last) in enumerate(spans(tokens, slot == len(offsets) - 1)):
            for member, buf, copy in zip((act_member, grad_member), (act_buf, grad_buf), copies[slot, part]):
                copy.wait()
                sums += jnp.dot(member[:, first:last], buf[slot, first:last], preferred_element_type=jnp.float32)
        outs[slot][...] = fold(sums / count, rows, kept, tail)


def spread_kernel(*refs):
    parts, out = refs[:-1], refs[-1]
    total = parts[0][...]
    for part in parts[1:]:
        total += part[...]
    total = total.astype(out.dtype)
    for g in range(out.shape[0]):
        out[g] = total


def factor_kernel(seq_count, total_seqs, kept, tail, near, far, act_out, grad_out, own, act_buf, grad_buf, act_sem, grad_sem):
    chunks, pairs = near.shape[0], near.shape[1]
    rows = 2 * seq_count
    width = kept + tail
    half = pairs * ROWS
    tile, piece = act_buf.shape[1:]

    def chunk(c):
        parts = []
        for ref in (near, far):
            block = ref[lax.rem(c + 1, chunks)]
            flat = block.reshape(half, kept)
            if tail:
                flat = jnp.concatenate([flat, unfold(block, rows, kept, tail).reshape(half, tail)], axis=1)
            parts.append(flat)
        return jnp.concatenate(parts, axis=0)

    seq = lax.axis_index("seq")
    own[...] = chunk(seq).astype(jnp.float32)
    first = (lax.axis_index("pair") * lax.axis_size("core") + lax.axis_index("core")) * tile
    span = max(tile, LANES)
    base = pl.multiple_of(first // LANES * LANES, LANES)
    left = own[:, pl.ds(base, span)]
    if tile < span:
        left = pltpu.roll(left, span - (first - base), 1)
    left = left.T[:tile]
    kind = lax.rem(lax.broadcasted_iota(jnp.int32, left.shape, 1), ROWS)
    act_left = jnp.where(kind < seq_count, left, 0.0)
    grad_left = jnp.where((kind >= seq_count) & (kind < rows), left, 0.0)
    left = jnp.concatenate([act_left, grad_left], axis=0).astype(jnp.bfloat16)
    copies = []
    for c in range(chunks):
        right = chunk(c)
        for part in range(width // piece):
            at = c * (width // piece) + part
            product = jnp.dot(left, right[:, part * piece : (part + 1) * piece], preferred_element_type=jnp.float32)
            product *= 1.0 / total_seqs
            act_buf[at] = product[:tile]
            grad_buf[at] = product[tile:]
            cols = pl.ds(at * piece, piece)
            pair = (
                pltpu.make_async_copy(act_buf.at[at], act_out.at[:, cols], act_sem.at[at]),
                pltpu.make_async_copy(grad_buf.at[at], grad_out.at[:, cols], grad_sem.at[at]),
            )
            for copy in pair:
                copy.start()
            copies.append(pair)
    for pair in copies:
        for copy in pair:
            copy.wait()


def local(activations, out_grads, lengths):
    chunks = lax.axis_size("seq")
    pairs = lax.axis_size("pair")
    cores = lax.axis_size("core")
    tokens, depth = activations.shape[1], activations.shape[2]
    seq_count = lengths.shape[1]
    width = depth // chunks
    slabs = len(TAPER)
    tile = depth // (chunks * pairs * cores)
    kept, tail = spare_split(2 * seq_count, width)
    vmem = pl.BlockSpec(memory_space=pltpu.VMEM)
    anywhere = pl.BlockSpec(memory_space=pl.ANY)
    held = [pltpu.with_memory_space_constraint(a, pltpu.HBM) for a in (activations, out_grads, lengths)]

    def segment_sums(offsets):
        count = len(offsets) * slabs
        return pl.pallas_call(
            functools.partial(segment_kernel, seq_count, chunks, offsets, slabs, kept, tail),
            out_shape=[jax.ShapeDtypeStruct((ROWS, kept), jnp.float32)] * len(offsets),
            in_specs=[anywhere] * 3,
            out_specs=[vmem] * len(offsets),
            scratch_shapes=[
                pltpu.VMEM((len(offsets), tokens, width), jnp.bfloat16),
                pltpu.VMEM((len(offsets), tokens, width), jnp.bfloat16),
                pltpu.SMEM(lengths.shape, jnp.int32),
                pltpu.SemaphoreType.DMA((count,)),
                pltpu.SemaphoreType.DMA((count,)),
                pltpu.SemaphoreType.DMA,
            ],
            compiler_params=pltpu.CompilerParams(vmem_limit_bytes=20 * MIB),
            cost_estimate=pl.CostEstimate(
                flops=4 * ROWS * tokens * width * len(offsets),
                bytes_accessed=4 * tokens * width * len(offsets),
                transcendentals=0,
            ),
            name="segment_sums",
        )(*held)

    offsets = list(range(chunks - 1, 0, -1))
    sent = segment_sums(offsets)
    arrived = []
    for offset, part in zip(offsets, sent):
        ring = [(i, partner(i, offset, chunks)) for i in range(chunks)]
        arrived.append(lax.ppermute(part, "seq", ring))
    arrived += segment_sums([0])

    spread = pl.pallas_call(
        spread_kernel,
        out_shape=jax.ShapeDtypeStruct((chunks * pairs, ROWS, kept), jnp.bfloat16),
        in_specs=[vmem] * chunks,
        out_specs=vmem,
        compiler_params=pltpu.CompilerParams(vmem_limit_bytes=8 * MIB),
        name="mean_rows",
    )(*arrived)

    order = [pairs - 1] + list(range(pairs - 1))
    members = [[(s * pairs + p) * cores + c for s in [chunks - 1] + list(range(chunks - 1)) for p in order] for c in range(cores)]
    near = lax.all_to_all(spread, ("seq", "pair", "core"), 0, 0, axis_index_groups=members, tiled=True)
    far = lax.ppermute(near, "core", [(i, (i + 1) % cores) for i in range(cores)])
    near, far = (a.reshape(chunks, pairs, ROWS, kept) for a in (near, far))

    piece = width // 2 if width % (2 * LANES) == 0 else width
    return pl.pallas_call(
        functools.partial(factor_kernel, seq_count, seq_count * pairs * cores, kept, tail),
        out_shape=[jax.ShapeDtypeStruct((tile, depth), jnp.float32)] * 2,
        in_specs=[vmem] * 2,
        out_specs=[anywhere] * 2,
        scratch_shapes=[
            pltpu.VMEM((2 * pairs * ROWS, width), jnp.float32),
            pltpu.VMEM((depth // piece, tile, piece), jnp.float32),
            pltpu.VMEM((depth // piece, tile, piece), jnp.float32),
            pltpu.SemaphoreType.DMA((depth // piece,)),
            pltpu.SemaphoreType.DMA((depth // piece,)),
        ],
        compiler_params=pltpu.CompilerParams(vmem_limit_bytes=20 * MIB),
        name="factor_tiles",
    )(near, far)


def solution(mesh):
    batch = mesh.shape["batch"]
    split = Mesh(mesh.devices.reshape(mesh.shape["seq"], batch // 2, 2), ("seq", "pair", "core"))
    groups = ("pair", "core")
    in_specs = (P(groups, "seq", None), P(groups, "seq", None), P(groups, None))
    out_specs = (P(("seq",) + groups, None), P(("seq",) + groups, None))

    def program(activations, out_grads, lengths):
        return tuple(jax.shard_map(local, mesh=split, in_specs=in_specs, out_specs=out_specs, check_vma=False)(activations, out_grads, lengths))

    return program
```

```python
import functools

import jax
import jax.numpy as jnp
from jax import lax
from jax.experimental import pallas as pl
from jax.experimental.pallas import tpu as pltpu
from jax.sharding import Mesh
from jax.sharding import PartitionSpec as P

LANES = 128
ROWS = 8
EVEN, TAPER = (1, 1), (3, 2, 1)
MIB = 1 << 20


def spare_split(rows, width):
    spare = ROWS - rows
    if spare <= 0 or rows % spare or (width * rows) % (ROWS * LANES):
        return width, 0
    kept = width * rows // ROWS
    tail = width - kept
    if tail % LANES:
        return width, 0
    return kept, tail


def spans(total, last):
    shares = TAPER if last else EVEN
    edges = [sum(shares[:i]) * total // sum(shares) // LANES * LANES for i in range(len(shares))] + [total]
    return [(a, b) for a, b in zip(edges, edges[1:]) if b > a]


def partner(index, offset, count):
    if count & (count - 1) == 0:
        return index ^ offset
    return (index + offset) % count


def fold(values, rows, kept, tail):
    if not tail:
        return values
    row = lax.broadcasted_iota(jnp.int32, (ROWS, 1), 0)
    spare = ROWS - rows
    per = rows // spare
    pieces = []
    for k in range(per):
        piece = values[:, k * tail : (k + 1) * tail]
        for j in range(spare):
            piece = jnp.where(row == rows + j, values[j * per + k : j * per + k + 1, kept:], piece)
        pieces.append(piece)
    return jnp.concatenate(pieces, axis=1)


def unfold(block, rows, kept, tail):
    row = lax.broadcasted_iota(jnp.int32, (1, ROWS, 1), 1)
    spare = ROWS - rows
    per = rows // spare
    wide = block.astype(jnp.float32)
    rest = jnp.zeros((block.shape[0], ROWS, tail), jnp.float32)
    for j in range(spare):
        for k in range(per):
            source = wide[:, rows + j : rows + j + 1, k * tail : (k + 1) * tail]
            rest = jnp.where(row == j * per + k, source, rest)
    return rest.astype(block.dtype)


def segment_kernel(seq_count, chunk_count, offsets, slabs, kept, tail, act, grad, lens, *refs):
    outs = refs[: len(offsets)]
    act_buf, grad_buf, len_buf, act_sem, grad_sem, len_sem = refs[len(offsets) :]
    tokens = act.shape[1]
    width = kept + tail
    rows = 2 * seq_count
    me = lax.axis_index("seq")
    len_copy = pltpu.make_async_copy(lens, len_buf, len_sem)
    len_copy.start()
    copies = {}
    for slot, offset in enumerate(offsets):
        base = partner(me, offset, chunk_count) * width
        cols = pl.ds(pl.multiple_of(base, width), width)
        for part, (first, last) in enumerate(spans(tokens, slot == len(offsets) - 1)):
            at = slot * slabs + part
            span = pl.ds(first, last - first)
            pair = (
                pltpu.make_async_copy(act.at[0, span, cols], act_buf.at[slot, span], act_sem.at[at]),
                pltpu.make_async_copy(grad.at[0, span, cols], grad_buf.at[slot, span], grad_sem.at[at]),
            )
            for copy in pair:
                copy.start()
            copies[slot, part] = pair
    len_copy.wait()
    row = lax.broadcasted_iota(jnp.int32, (ROWS, tokens), 0)
    position = lax.broadcasted_iota(jnp.int32, (ROWS, tokens), 1) + me * tokens
    thin = lax.broadcasted_iota(jnp.int32, (ROWS, 1), 0)
    low = jnp.zeros((ROWS, tokens), jnp.int32)
    high = jnp.zeros((ROWS, tokens), jnp.int32)
    count = jnp.ones((ROWS, 1), jnp.float32)
    start = jnp.int32(0)
    for s in range(seq_count):
        size = len_buf[0, s]
        mine = (row == s) | (row == s + seq_count)
        low = jnp.where(mine, start, low)
        high = jnp.where(mine, start + size, high)
        count = jnp.where(thin == s, size.astype(jnp.float32), count)
        start = start + size
    member = (position >= low) & (position < high)
    act_member = jnp.where(member & (row < seq_count), 1.0, 0.0).astype(jnp.bfloat16)
    grad_member = jnp.where(member & (row >= seq_count), 1.0, 0.0).astype(jnp.bfloat16)
    for slot in range(len(offsets)):
        sums = jnp.zeros((ROWS, width), jnp.float32)
        for part, (first, last) in enumerate(spans(tokens, slot == len(offsets) - 1)):
            for member, buf, copy in zip((act_member, grad_member), (act_buf, grad_buf), copies[slot, part]):
                copy.wait()
                sums += jnp.dot(member[:, first:last], buf[slot, first:last], preferred_element_type=jnp.float32)
        outs[slot][...] = fold(sums / count, rows, kept, tail)


def spread_kernel(*refs):
    parts, out = refs[:-1], refs[-1]
    total = parts[0][...]
    for part in parts[1:]:
        total += part[...]
    total = total.astype(out.dtype)
    for g in range(out.shape[0]):
        out[g] = total


def factor_kernel(seq_count, total_seqs, kept, tail, near, far, act_out, grad_out, own, act_buf, grad_buf, act_sem, grad_sem):
    chunks, pairs = near.shape[0], near.shape[1]
    rows = 2 * seq_count
    width = kept + tail
    half = pairs * ROWS
    tile, piece = act_buf.shape[1:]

    def chunk(c):
        parts = []
        for ref in (near, far):
            block = ref[lax.rem(c + 1, chunks)]
            flat = block.reshape(half, kept)
            if tail:
                flat = jnp.concatenate([flat, unfold(block, rows, kept, tail).reshape(half, tail)], axis=1)
            parts.append(flat)
        return jnp.concatenate(parts, axis=0)

    seq = lax.axis_index("seq")
    own[...] = chunk(seq).astype(jnp.float32)
    first = (lax.axis_index("pair") * lax.axis_size("core") + lax.axis_index("core")) * tile
    span = max(tile, LANES)
    base = pl.multiple_of(first // LANES * LANES, LANES)
    left = own[:, pl.ds(base, span)]
    if tile < span:
        left = pltpu.roll(left, span - (first - base), 1)
    left = left.T[:tile]
    kind = lax.rem(lax.broadcasted_iota(jnp.int32, left.shape, 1), ROWS)
    act_left = jnp.where(kind < seq_count, left, 0.0)
    grad_left = jnp.where((kind >= seq_count) & (kind < rows), left, 0.0)
    left = jnp.concatenate([act_left, grad_left], axis=0).astype(jnp.bfloat16)
    copies = []
    for c in range(chunks):
        right = chunk(c)
        for part in range(width // piece):
            at = c * (width // piece) + part
            product = jnp.dot(left, right[:, part * piece : (part + 1) * piece], preferred_element_type=jnp.float32)
            product *= 1.0 / total_seqs
            act_buf[at] = product[:tile]
            grad_buf[at] = product[tile:]
            cols = pl.ds(at * piece, piece)
            pair = (
                pltpu.make_async_copy(act_buf.at[at], act_out.at[:, cols], act_sem.at[at]),
                pltpu.make_async_copy(grad_buf.at[at], grad_out.at[:, cols], grad_sem.at[at]),
            )
            for i, copy in enumerate(pair):
                copy.start(priority=i)
            copies.append(pair)
    for pair in copies:
        for copy in pair:
            copy.wait()


def local(activations, out_grads, lengths):
    chunks = lax.axis_size("seq")
    pairs = lax.axis_size("pair")
    cores = lax.axis_size("core")
    tokens, depth = activations.shape[1], activations.shape[2]
    seq_count = lengths.shape[1]
    width = depth // chunks
    slabs = len(TAPER)
    tile = depth // (chunks * pairs * cores)
    kept, tail = spare_split(2 * seq_count, width)
    vmem = pl.BlockSpec(memory_space=pltpu.VMEM)
    anywhere = pl.BlockSpec(memory_space=pl.ANY)
    held = [pltpu.with_memory_space_constraint(a, pltpu.HBM) for a in (activations, out_grads, lengths)]

    def segment_sums(offsets):
        count = len(offsets) * slabs
        return pl.pallas_call(
            functools.partial(segment_kernel, seq_count, chunks, offsets, slabs, kept, tail),
            out_shape=[jax.ShapeDtypeStruct((ROWS, kept), jnp.float32)] * len(offsets),
            in_specs=[anywhere] * 3,
            out_specs=[vmem] * len(offsets),
            scratch_shapes=[
                pltpu.VMEM((len(offsets), tokens, width), jnp.bfloat16),
                pltpu.VMEM((len(offsets), tokens, width), jnp.bfloat16),
                pltpu.SMEM(lengths.shape, jnp.int32),
                pltpu.SemaphoreType.DMA((count,)),
                pltpu.SemaphoreType.DMA((count,)),
                pltpu.SemaphoreType.DMA,
            ],
            compiler_params=pltpu.CompilerParams(vmem_limit_bytes=20 * MIB),
            cost_estimate=pl.CostEstimate(
                flops=4 * ROWS * tokens * width * len(offsets),
                bytes_accessed=4 * tokens * width * len(offsets),
                transcendentals=0,
            ),
            name="segment_sums",
        )(*held)

    offsets = list(range(chunks - 1, 0, -1))
    sent = segment_sums(offsets)
    arrived = []
    for offset, part in zip(offsets, sent):
        ring = [(i, partner(i, offset, chunks)) for i in range(chunks)]
        arrived.append(lax.ppermute(part, "seq", ring))
    arrived += segment_sums([0])

    spread = pl.pallas_call(
        spread_kernel,
        out_shape=jax.ShapeDtypeStruct((chunks * pairs, ROWS, kept), jnp.bfloat16),
        in_specs=[vmem] * chunks,
        out_specs=vmem,
        compiler_params=pltpu.CompilerParams(vmem_limit_bytes=8 * MIB),
        name="mean_rows",
    )(*arrived)

    order = [pairs - 1] + list(range(pairs - 1))
    members = [[(s * pairs + p) * cores + c for s in [chunks - 1] + list(range(chunks - 1)) for p in order] for c in range(cores)]
    near = lax.all_to_all(spread, ("seq", "pair", "core"), 0, 0, axis_index_groups=members, tiled=True)
    far = lax.ppermute(near, "core", [(i, (i + 1) % cores) for i in range(cores)])
    near, far = (a.reshape(chunks, pairs, ROWS, kept) for a in (near, far))

    piece = width // 2 if width % (2 * LANES) == 0 else width
    return pl.pallas_call(
        functools.partial(factor_kernel, seq_count, seq_count * pairs * cores, kept, tail),
        out_shape=[jax.ShapeDtypeStruct((tile, depth), jnp.float32)] * 2,
        in_specs=[vmem] * 2,
        out_specs=[anywhere] * 2,
        scratch_shapes=[
            pltpu.VMEM((2 * pairs * ROWS, width), jnp.float32),
            pltpu.VMEM((depth // piece, tile, piece), jnp.float32),
            pltpu.VMEM((depth // piece, tile, piece), jnp.float32),
            pltpu.SemaphoreType.DMA((depth // piece,)),
            pltpu.SemaphoreType.DMA((depth // piece,)),
        ],
        compiler_params=pltpu.CompilerParams(vmem_limit_bytes=20 * MIB),
        name="factor_tiles",
    )(near, far)


def solution(mesh):
    batch = mesh.shape["batch"]
    split = Mesh(mesh.devices.reshape(mesh.shape["seq"], batch // 2, 2), ("seq", "pair", "core"))
    groups = ("pair", "core")
    in_specs = (P(groups, "seq", None), P(groups, "seq", None), P(groups, None))
    out_specs = (P(("seq",) + groups, None), P(("seq",) + groups, None))

    def program(activations, out_grads, lengths):
        return tuple(jax.shard_map(local, mesh=split, in_specs=in_specs, out_specs=out_specs, check_vma=False)(activations, out_grads, lengths))

    return program
```
